32 devices in a mesh: parts: 2 (over y), row: 8 (over z, core), col: 2 (over x), sub: 1.
Axes of the slice: x: 2, y: 2, z: 4, core: 2. Of those that a mesh axis runs over, the one named last changes fastest.
Arguments:
- pair: float32 [192, 96, 128], P(('parts', 'row'), ('col', 'sub')), parts along dimension 0, may hold values from -250 to 250, as said below
- residue_mask: int32 [192], P('parts'), parts along dimension 0, may hold values from 0 to 1, as said below
- tri_norm_gain: float32 [128], replicated, may hold values from 0.25 to 1.75
- tri_in_weight: bfloat16 [128, 4, 128], replicated, may hold values from -0.5 to 0.5
- tri_gate_weight: bfloat16 [128, 128], replicated, may hold values from -0.5 to 0.5
- tri_out_norm_gain: float32 [128], replicated, may hold values from 0.25 to 1.75
- tri_out_weight: bfloat16 [128, 128], replicated, may hold values from -0.5 to 0.5
- att_norm_gain: float32 [128], replicated, may hold values from 0.25 to 1.75
- att_proj_weight: bfloat16 [128, 4, 128], replicated, may hold values from -0.5 to 0.5
- att_bias_weight: bfloat16 [128, 4], replicated, may hold values from -15 to 15
- att_out_weight: bfloat16 [128, 128], replicated, may hold values from -0.5 to 0.5
Outputs:
- pair_out: float32 [192, 96, 128], P(('parts', 'row'), ('col', 'sub')), parts along dimension 0
The draws below stay inside these ranges and needn't reach their ends.
There are 2 independent parts, one for each index of `parts`. The reference program is written for one: setup_inputs(seed, part) draws one part's arguments, and reference() takes and returns one part's arrays. A program takes and returns all parts, laid end to end along the dimension named above; an argument that names none is the same for every part. Nothing has to cross between parts.
Inputs may be any that keep to these rules, and one draw needn't show every extreme that they name: The pair entries are finite. `residue_mask`: 0 on every residue at or above a length of at least 48 and less than 96; below it 1, except some unresolved residues that are 0; residue 0 is always 1.
All inputs are finite; a program needn't handle non-finite values.
Results may differ from the reference program's by a relative error of at most 0.0032.
Values may be sent and summed in bfloat16 or wider, within the bound.
A program may use at most 64 MiB of HBM per device.

```python
import math
import jax
import jax.numpy as jnp
from jax import lax

PAIR_CH = 128
TRI_HID = 128
HEADS = 4
HEAD_DIM = 32
RESIDUES = 96


def draw_pair(key, part):
    base_draw = jnp.clip(jax.random.normal(key, (RESIDUES, RESIDUES, PAIR_CH), jnp.float32), -6.0, 6.0)
    return base_draw


def draw_residue_mask(key, part):
    length = jax.random.randint(jax.random.fold_in(key, 7), (), RESIDUES // 2, RESIDUES)
    kept = jax.random.randint(jax.random.fold_in(key, 8), (RESIDUES,), 0, 8) != 0
    positions = jnp.arange(RESIDUES)
    live = (positions < length) & (kept | (positions == 0))
    return live.astype(jnp.int32)


def draw_att_bias_weight(key, part):
    base_draw = jnp.clip(jax.random.normal(key, (PAIR_CH, HEADS), jnp.float32), -4.0, 4.0)
    spread = 2.0
    return jnp.clip(base_draw * (spread / math.sqrt(PAIR_CH)), -15.0, 15.0).astype(jnp.bfloat16)


def gaussian(own_key, extent, scale, most, dtype=jnp.bfloat16):
    entries = jax.random.normal(own_key, extent, jnp.float32) * scale
    return jnp.minimum(jnp.maximum(entries, -most), most).astype(dtype)


def setup_inputs(seed: int = 0, part: int = 0) -> dict:
    streams_of = jax.random.split(jax.random.key(seed), 12)
    part_keys = jax.random.split(jax.random.fold_in(streams_of[11], part), 12)
    return {
        "pair": draw_pair(jax.random.fold_in(jax.random.fold_in(streams_of[11], part), 71), part),
        "residue_mask": draw_residue_mask(jax.random.fold_in(jax.random.fold_in(streams_of[11], part), 71), part),
        "tri_norm_gain": jnp.clip(1.0 + 0.15 * jax.random.normal(streams_of[2], (PAIR_CH,), jnp.float32), 0.25, 1.75),
        "tri_in_weight": gaussian(streams_of[3], (PAIR_CH, 4, TRI_HID), PAIR_CH ** -0.5, 0.5),
        "tri_gate_weight": gaussian(streams_of[4], (PAIR_CH, PAIR_CH), PAIR_CH ** -0.5, 0.5),
        "tri_out_norm_gain": jnp.clip(1.0 + 0.15 * jax.random.normal(streams_of[5], (TRI_HID,), jnp.float32), 0.25, 1.75),
        "tri_out_weight": gaussian(streams_of[6], (TRI_HID, PAIR_CH), TRI_HID ** -0.5, 0.5),
        "att_norm_gain": jnp.clip(1.0 + 0.15 * jax.random.normal(streams_of[7], (PAIR_CH,), jnp.float32), 0.25, 1.75),
        "att_proj_weight": gaussian(streams_of[8], (PAIR_CH, 4, HEADS * HEAD_DIM), PAIR_CH ** -0.5, 0.5),
        "att_bias_weight": draw_att_bias_weight(jax.random.fold_in(streams_of[11], 71), part),
        "att_out_weight": gaussian(streams_of[10], (HEADS * HEAD_DIM, PAIR_CH), (HEADS * HEAD_DIM) ** -0.5, 0.5),
    }


epsilon = 1e-05
mask_penalty = 1000000000.0

def norm_last(values_in, gain):
    center = lax.optimization_barrier(jnp.mean(values_in, axis=-1, keepdims=True))
    centered = values_in - center
    variance = lax.optimization_barrier(jnp.mean(centered * centered, axis=-1, keepdims=True))
    return centered * lax.rsqrt(variance + epsilon) * gain

def project(normed, weight):
    flat_rows = normed.reshape(-1, normed.shape[-1])
    product = jnp.dot(flat_rows, weight, preferred_element_type=jnp.float32)
    return product.reshape(normed.shape[:-1] + (weight.shape[1],))

def reference(pair, residue_mask, tri_norm_gain, tri_in_weight, tri_gate_weight, tri_out_norm_gain, tri_out_weight, att_norm_gain, att_proj_weight, att_bias_weight, att_out_weight):
    residue_live = residue_mask.astype(jnp.float32)
    pair_live = (residue_live[:, None] * residue_live[None, :])[:, :, None]
    tri_normed = norm_last(pair, tri_norm_gain).astype(jnp.bfloat16)
    left_factor = (jax.nn.sigmoid(project(tri_normed, tri_in_weight[:, 0])) * project(tri_normed, tri_in_weight[:, 1]) * pair_live).astype(jnp.bfloat16)
    right_factor = (jax.nn.sigmoid(project(tri_normed, tri_in_weight[:, 2])) * project(tri_normed, tri_in_weight[:, 3]) * pair_live).astype(jnp.bfloat16)
    tri_sum = jnp.einsum('ikh,jkh->ijh', left_factor.astype(jnp.float32), right_factor.astype(jnp.float32))
    hidden_normed = norm_last(tri_sum, tri_out_norm_gain).astype(jnp.bfloat16)
    tri_gate = jax.nn.sigmoid(project(tri_normed, tri_gate_weight))
    pair_mid = pair + tri_gate * project(hidden_normed, tri_out_weight)
    att_normed = norm_last(pair_mid, att_norm_gain).astype(jnp.bfloat16)
    head_shape = (RESIDUES, RESIDUES, HEADS, HEAD_DIM)
    queries = (project(att_normed, att_proj_weight[:, 0]) * HEAD_DIM ** (-0.5)).astype(jnp.bfloat16).reshape(head_shape)
    key_rows = project(att_normed, att_proj_weight[:, 1]).astype(jnp.bfloat16).reshape(head_shape)
    value_rows = project(att_normed, att_proj_weight[:, 2]).astype(jnp.bfloat16).reshape(head_shape)
    att_gate = jax.nn.sigmoid(project(att_normed, att_proj_weight[:, 3]))
    pair_bias = project(att_normed, att_bias_weight).astype(jnp.bfloat16)
    mask_row = (residue_live - 1.0) * mask_penalty
    head_bias = jnp.transpose(pair_bias.astype(jnp.float32), (2, 0, 1)) + mask_row[None, None, :]

    def one_row(row_item):
        query_row, key_row, value_row = row_item
        scores = jnp.einsum('jhd,khd->hjk', query_row.astype(jnp.float32), key_row.astype(jnp.float32)) + head_bias
        row_max = lax.optimization_barrier(jnp.max(scores, axis=-1, keepdims=True))
        raised = jnp.exp(scores - row_max)
        weights = (raised / lax.optimization_barrier(jnp.sum(raised, axis=-1, keepdims=True))).astype(jnp.bfloat16)
        return jnp.einsum('hjk,khd->jhd', weights.astype(jnp.float32), value_row.astype(jnp.float32))
    attended = lax.map(one_row, (queries, key_rows, value_rows))
    gated = (attended.reshape(RESIDUES, RESIDUES, HEADS * HEAD_DIM) * att_gate).astype(jnp.bfloat16)
    return pair_mid + project(gated, att_out_weight)
```

```python
import functools
import math

import jax
import jax.numpy as jnp
from jax import lax
from jax.experimental import pallas as pl
from jax.experimental.pallas import tpu as pltpu
from jax.sharding import PartitionSpec as P

epsilon = 1e-05
mask_penalty = 1000000000.0
MESH = pl.DeviceIdType.MESH
F32 = jnp.float32
BF16 = jnp.bfloat16


def norm_last(values_in, gain):
    center = jnp.mean(values_in, axis=-1, keepdims=True)
    centered = values_in - center
    variance = jnp.mean(centered * centered, axis=-1, keepdims=True)
    return centered * lax.rsqrt(variance + epsilon) * gain


def dot(a, b):
    return jnp.dot(a, b, preferred_element_type=F32)


def dot_nt(a, b):
    return lax.dot_general(a, b, (((1,), (1,)), ((), ())), preferred_element_type=F32)


def fold_sublanes(parts):
    lane_row = lax.broadcasted_iota(jnp.int32, parts[0].shape, 0)
    for width in (4, 2, 1):
        low = (lane_row & width) == 0
        half = len(parts) // 2
        folded = []
        for u in range(half):
            x, y = parts[u], parts[u + half]
            if width == 4:
                folded.append(jnp.where(low, x, y) + pltpu.roll(jnp.where(low, y, x), 4, 0))
            else:
                folded.append(
                    jnp.where(low, x, y)
                    + jnp.where(low, pltpu.roll(x, 8 - width, 0), pltpu.roll(y, width, 0))
                )
        parts = folded
    return parts[0]


def kernel(
    dims,
    pair_ref, mask_ref, g1_ref, w_in_ref, w_gate_ref, g2_ref, w_out_ref, g3_ref, w_att_ref, w_bias_ref, w_o_ref,
    out_ref,
    live_s, normed_s, right_all, left_s, gate_s, rf_s, part_s, part_in, sum_s, tri_s, mid_s,
    att_all, q_s, ag_s, k_s, v_s, bias_f, bias_own, bias_all, bfull,
    rs_send, rs_recv, ps_send, ps_recv, as_send, as_recv, bs_send, bs_recv,
):
    nrow, ncol, nsub, group = dims
    rows, cols, chan = pair_ref.shape
    cc = ncol * nsub
    residues = cols * cc
    rb = nrow // cc
    nz = nrow // group
    hid = w_gate_ref.shape[1]
    heads = bias_f.shape[0]
    head_size = hid // heads
    ch = next(n for n in (4, 2, 1) if rows % n == 0)
    nt = rows // ch

    r = lax.axis_index("row")
    c = lax.axis_index("col") * nsub + lax.axis_index("sub")
    z = r // group
    p = r % group

    def at(row, cc_index):
        return {"row": row, "col": cc_index // nsub, "sub": cc_index % nsub}

    barrier = pltpu.get_barrier_semaphore()
    me = r * cc + c

    @pl.loop(1, nrow * cc)
    def _(n):
        other = (me + n) % (nrow * cc)
        pl.semaphore_signal(barrier, inc=1, device_id=at(other // cc, other % cc), device_id_type=MESH)

    live = mask_ref[...].astype(F32)
    eye = lax.broadcasted_iota(jnp.int32, (residues, residues), 0) == lax.broadcasted_iota(
        jnp.int32, (residues, residues), 1
    )
    column = jnp.sum(jnp.where(eye, jnp.broadcast_to(live, (residues, residues)), 0.0), axis=1, keepdims=True)
    live_s[...] = jnp.broadcast_to(column, live_s.shape)
    live_cols = live_s[pl.ds(pl.multiple_of(c * cols, 8), cols), :]

    def right_copy(way, slot, t):
        target = (r + group, r - group, z * group + (group - 1 - p))[way]
        piece = right_all.at[slot, pl.ds(t * ch, ch)]
        return pltpu.make_async_remote_copy(
            src_ref=piece, dst_ref=piece,
            send_sem=rs_send.at[way, slot, t], recv_sem=rs_recv.at[slot, t],
            device_id={"row": target}, device_id_type=MESH,
        )

    for t in range(nt):
        sl = slice(t * ch, (t + 1) * ch)
        normed = norm_last(pair_ref[sl].reshape(ch * cols, chan), g1_ref[...]).astype(BF16)
        normed_s[t] = normed
        proj = dot(normed, w_in_ref[:, 2 * hid :])
        prod = (jax.nn.sigmoid(proj[:, :hid]) * proj[:, hid:]).reshape(ch, cols, hid)
        for u in range(ch):
            both = live_cols * live_s[pl.ds(r * rows + t * ch + u, 1), :]
            right_all[r, t * ch + u] = (prod[u] * both).astype(BF16)
        if t == 0:
            pl.semaphore_wait(barrier, nrow * cc - 1)

        @pl.when(z + 1 < nz)
        def _():
            right_copy(0, r, t).start()

        @pl.when(z >= 1)
        def _():
            right_copy(1, r, t).start()

        if group == 2:
            right_copy(2, r, t).start()

    for t in range(nt):
        proj = dot(normed_s[t], w_in_ref[:, : 2 * hid])
        prod = (jax.nn.sigmoid(proj[:, :hid]) * proj[:, hid:]).reshape(ch, cols, hid)
        gate_s[t] = jax.nn.sigmoid(dot(normed_s[t], w_gate_ref[...]))
        for u in range(ch):
            both = live_cols * live_s[pl.ds(r * rows + t * ch + u, 1), :]
            left_s[t * ch + u] = (prod[u] * both).astype(BF16).astype(F32)

    ig = next(n for n in range(1, 9) if (n * rows) % 8 == 0 and rows % n == 0)

    def part_copy(slot):
        return pltpu.make_async_remote_copy(
            src_ref=part_s.at[slot], dst_ref=part_in.at[c, slot % rb],
            send_sem=ps_send.at[slot], recv_sem=ps_recv.at[c, slot % rb],
            device_id=at(r, slot // rb), device_id_type=MESH,
        )

    def compute(slot):
        rf_s[...] = right_all[slot].astype(F32)

        @pl.loop(0, rows // ig)
        def _(ip):
            accs = [None] * (ig * rows)
            for kv in range(cols // 8):
                ks = slice(kv * 8, kv * 8 + 8)
                lefts = [left_s[ip * ig + u, ks, :] for u in range(ig)]
                for j in range(rows):
                    rv = rf_s[j, ks, :]
                    for u in range(ig):
                        n = u * rows + j
                        term = lefts[u] * rv
                        accs[n] = term if accs[n] is None else accs[n] + term
            for n in range(ig * rows // 8):
                start = pl.multiple_of(ip * (ig * rows) + n * 8, 8)
                part_s[slot, pl.ds(start, 8), :] = fold_sublanes(accs[n * 8 : n * 8 + 8])

        @pl.when(slot // rb != c)
        def _():
            part_copy(slot).start()

    def event(n):
        away = (n + 1) // 2
        return jnp.where(n % 2 == 1, z - away, z + away)

    @pl.loop(1, 2 * nz)
    def _(n):
        zn = event(n)

        @pl.when((zn >= 0) & (zn < nz))
        def _():
            slot = zn * group + p
            for t in range(nt):
                right_copy(0, slot, t).wait_recv()

                @pl.when((zn < z) & (z + 1 < nz))
                def _():
                    right_copy(0, slot, t).start()

                @pl.when((zn > z) & (z >= 1))
                def _():
                    right_copy(1, slot, t).start()

                if group == 2:
                    right_copy(2, slot, t).start()

        zp = event(n - 1)

        @pl.when((zp >= 0) & (zp < nz))
        def _():
            @pl.loop(0, group)
            def _(q):
                slot = zp * group + (p + q) % group

                @pl.when(q == 1)
                def _():
                    for t in range(nt):
                        right_copy(2, slot, t).wait_recv()

                compute(slot)

    for b in range(rb):
        total = part_s[c * rb + b]
        for away in range(1, cc):
            source = (c + away) % cc
            pltpu.make_async_remote_copy(
                src_ref=part_s.at[0], dst_ref=part_in.at[source, b],
                send_sem=ps_send.at[0], recv_sem=ps_recv.at[source, b],
                device_id=at(r, source), device_id_type=MESH,
            ).wait_recv()
            total = total + part_in[source, b]
        sum_s[b] = total
        for i in range(rows):
            tri_s[i, b * rows : (b + 1) * rows, :] = sum_s[b, i * rows : (i + 1) * rows, :]

    def att_copy(t, away, source):
        piece = att_all.at[source, pl.ds(t * ch, ch)]
        return pltpu.make_async_remote_copy(
            src_ref=piece, dst_ref=piece,
            send_sem=as_send.at[away, t], recv_sem=as_recv.at[source, t],
            device_id=at(r, (c + away) % cc), device_id_type=MESH,
        )

    bias_f[...] = jnp.zeros_like(bias_f)
    for t in range(nt):
        sl = slice(t * ch, (t + 1) * ch)
        hidden = norm_last(tri_s[sl].reshape(ch * cols, hid), g2_ref[...]).astype(BF16)
        mid = pair_ref[sl].reshape(ch * cols, chan) + gate_s[t] * dot(hidden, w_out_ref[...])
        mid_s[t] = mid
        att = norm_last(mid, g3_ref[...]).astype(BF16)
        att_all[c, sl] = att.reshape(ch, cols, chan)
        for away in range(1, cc):
            att_copy(t, away, c).start()
        for u in range(ch):
            heads_first = dot_nt(w_bias_ref[...], att[u * cols : (u + 1) * cols])
            for h in range(heads):
                bias_f[h, t * ch + u : t * ch + u + 1, :] = heads_first[h : h + 1, :]

    bias_own[...] = bias_f[...].astype(BF16)
    panel = r // rb

    def bias_copy(row, source_c, source_b):
        return pltpu.make_async_remote_copy(
            src_ref=bias_own, dst_ref=bias_all.at[source_c, source_b],
            send_sem=bs_send.at[row], recv_sem=bs_recv.at[source_c, source_b],
            device_id=at(row, panel), device_id_type=MESH,
        )

    @pl.loop(0, nrow)
    def _(n):
        row = (r + n) % nrow

        @pl.when((n > 0) | (panel != c))
        def _():
            bias_copy(row, c, r % rb).start()

    @pl.when(panel == c)
    def _():
        bias_all[c, r % rb] = bias_f[...].astype(BF16)

    for t in range(nt):
        sl = slice(t * ch, (t + 1) * ch)
        att = att_all[c, sl].reshape(ch * cols, chan)
        proj = dot(att, w_att_ref[...])
        q_s[sl] = (proj[:, :hid] * head_size ** (-0.5)).astype(BF16).reshape(ch, cols, hid)
        k_s[c, sl] = proj[:, hid : 2 * hid].astype(BF16).reshape(ch, cols, hid)
        v_s[c, sl] = proj[:, 2 * hid : 3 * hid].astype(BF16).reshape(ch, cols, hid)
        ag_s[sl] = jax.nn.sigmoid(proj[:, 3 * hid :]).reshape(ch, cols, hid)

    for away in range(1, cc):
        source = (c + away) % cc
        for t in range(nt):
            sl = slice(t * ch, (t + 1) * ch)
            att_copy(t, away, source).wait_recv()
            att = att_all[source, sl].reshape(ch * cols, chan)
            proj = dot(att, w_att_ref[:, hid : 3 * hid])
            k_s[source, sl] = proj[:, :hid].astype(BF16).reshape(ch, cols, hid)
            v_s[source, sl] = proj[:, hid:].astype(BF16).reshape(ch, cols, hid)

    mask_row = (live - 1.0) * mask_penalty
    for source in range(cc):
        for b in range(rb):
            @pl.when((c != source) | (r != c * rb + b))
            def _():
                bias_copy(r, source, b).wait_recv()

            for h in range(heads):
                bfull[h, b * rows : (b + 1) * rows, source * cols : (source + 1) * cols] = (
                    bias_all[source, b, h].astype(F32)[:rows] + mask_row[:, source * cols : (source + 1) * cols]
                )

    head_of = lax.broadcasted_iota(jnp.int32, (cols, hid), 1) // head_size
    ones = jnp.ones((residues, hid), BF16)

    @pl.loop(0, nt)
    def _(t):
        gated = []
        for u in range(ch):
            i = t * ch + u
            query = q_s[i]
            stacked = jnp.concatenate(
                [jnp.where(head_of == h, query, jnp.zeros_like(query)) for h in range(heads)], axis=0
            )
            keys = jnp.concatenate([k_s[s, i] for s in range(cc)], axis=0)
            values = jnp.concatenate([v_s[s, i] for s in range(cc)], axis=0)
            scores = dot_nt(stacked, keys) + bfull[...].reshape(heads * cols, residues)
            raised = jnp.exp(scores - jnp.max(scores, axis=-1, keepdims=True)).astype(BF16)
            both = dot(raised, jnp.concatenate([values, ones], axis=1))
            top, bottom = both[:cols, :hid], both[:cols, hid:]
            for h in range(1, heads):
                rows_h = both[h * cols : (h + 1) * cols]
                top = jnp.where(head_of == h, rows_h[:, :hid], top)
                bottom = jnp.where(head_of == h, rows_h[:, hid:], bottom)
            gated.append((top / bottom * ag_s[i]).astype(BF16))
        result = mid_s[t] + dot(jnp.concatenate(gated, axis=0), w_o_ref[...])
        out_ref[pl.ds(t * ch, ch)] = result.reshape(ch, cols, chan)

    @pl.loop(0, nrow)
    def _(slot):
        zn, pn = slot // group, slot % group

        @pl.when(pn == p)
        def _():
            for t in range(nt):
                @pl.when((zn <= z) & (z + 1 < nz))
                def _():
                    right_copy(0, slot, t).wait_send()

                @pl.when((zn >= z) & (z >= 1))
                def _():
                    right_copy(1, slot, t).wait_send()

                if group == 2:
                    right_copy(2, slot, t).wait_send()

        @pl.when(slot // rb != c)
        def _():
            part_copy(slot).wait_send()

        @pl.when((slot != r) | (panel != c))
        def _():
            bias_copy(slot, c, r % rb).wait_send()

    for away in range(1, cc):
        for t in range(nt):
            att_copy(t, away, c).wait_send()


def body(dims, pair, residue_mask, g1, w_in, w_gate, g2, w_out, g3, w_att, w_bias, w_o):
    nrow, ncol, nsub, group = dims
    rows, cols, chan = pair.shape
    cc = ncol * nsub
    residues = cols * cc
    rb = nrow // cc
    hid = w_in.shape[2]
    heads = w_bias.shape[1]
    ch = next(n for n in (4, 2, 1) if rows % n == 0)
    nt = rows // ch
    pad = -(-rows // 16) * 16
    bias_rows = jnp.pad(w_bias.T, ((0, -heads % 16), (0, 0)))
    V = pltpu.VMEM
    DMA = pltpu.SemaphoreType.DMA
    return pl.pallas_call(
        functools.partial(kernel, dims),
        out_shape=jax.ShapeDtypeStruct(pair.shape, F32),
        in_specs=[pl.BlockSpec(memory_space=pltpu.VMEM)] * 11,
        out_specs=pl.BlockSpec(memory_space=pltpu.VMEM),
        scratch_shapes=[
            V((residues, hid), F32),
            V((nt, ch * cols, chan), BF16),
            V((nrow, rows, cols, hid), BF16),
            V((rows, cols, hid), F32),
            V((nt, ch * cols, chan), F32),
            V((rows, cols, hid), F32),
            V((nrow, rows * rows, hid), F32),
            V((cc, rb, rows * rows, hid), F32),
            V((rb, rows * rows, hid), F32),
            V((rows, cols, hid), F32),
            V((nt, ch * cols, chan), F32),
            V((cc, rows, cols, chan), BF16),
            V((rows, cols, hid), BF16),
            V((rows, cols, hid), F32),
            V((cc, rows, cols, hid), BF16),
            V((cc, rows, cols, hid), BF16),
            V((heads, pad, cols), F32),
            V((heads, pad, cols), BF16),
            V((cc, rb, heads, pad, cols), BF16),
            V((heads, cols, residues), F32),
            DMA((3, nrow, nt)),
            DMA((nrow, nt)),
            DMA((nrow,)),
            DMA((cc, rb)),
            DMA((cc, nt)),
            DMA((cc, nt)),
            DMA((nrow,)),
            DMA((cc, rb)),
        ],
        compiler_params=pltpu.CompilerParams(
            collective_id=0, has_side_effects=True, vmem_limit_bytes=56 * 1024 * 1024
        ),
        name="pair_update",
    )(
        pair,
        residue_mask.reshape(1, -1),
        g1.reshape(1, -1),
        w_in.reshape(chan, -1),
        w_gate,
        g2.reshape(1, -1),
        w_out,
        g3.reshape(1, -1),
        w_att.reshape(chan, -1),
        bias_rows,
        w_o,
    )


def solution(mesh):
    shape = mesh.shape
    group = 2 if shape["sub"] == 1 and shape["row"] % 2 == 0 else 1
    dims = (shape["row"], shape["col"], shape["sub"], group)
    placed = (P(("parts", "row"), ("col", "sub"), None), P("parts")) + (P(),) * 9
    return jax.shard_map(
        functools.partial(body, dims),
        mesh=mesh,
        in_specs=placed,
        out_specs=P(("parts", "row"), ("col", "sub"), None),
        check_vma=False,
    )
```

```python
import functools
import math

import jax
import jax.numpy as jnp
from jax import lax
from jax.experimental import pallas as pl
from jax.experimental.pallas import tpu as pltpu
from jax.sharding import PartitionSpec as P

epsilon = 1e-05
mask_penalty = 1000000000.0
MESH = pl.DeviceIdType.MESH
F32 = jnp.float32
BF16 = jnp.bfloat16


def norm_last(values_in, gain):
    center = jnp.mean(values_in, axis=-1, keepdims=True)
    centered = values_in - center
    variance = jnp.mean(centered * centered, axis=-1, keepdims=True)
    return centered * lax.rsqrt(variance + epsilon) * gain


def dot(a, b):
    return jnp.dot(a, b, preferred_element_type=F32)


def dot_nt(a, b):
    return lax.dot_general(a, b, (((1,), (1,)), ((), ())), preferred_element_type=F32)


def fold_sublanes(parts):
    lane_row = lax.broadcasted_iota(jnp.int32, parts[0].shape, 0)
    for width in (4, 2, 1):
        low = (lane_row & width) == 0
        half = len(parts) // 2
        folded = []
        for u in range(half):
            x, y = parts[u], parts[u + half]
            if width == 4:
                folded.append(jnp.where(low, x, y) + pltpu.roll(jnp.where(low, y, x), 4, 0))
            else:
                folded.append(
                    jnp.where(low, x, y)
                    + jnp.where(low, pltpu.roll(x, 8 - width, 0), pltpu.roll(y, width, 0))
                )
        parts = folded
    return parts[0]


def kernel(
    dims,
    pair_ref, mask_ref, g1_ref, w_in_ref, w_gate_ref, g2_ref, w_out_ref, g3_ref, w_att_ref, w_bias_ref, w_o_ref,
    out_ref,
    live_s, normed_s, right_all, left_s, gate_s, rf_s, part_s, part_in, sum_s, tri_s, mid_s,
    att_all, q_s, ag_s, k_s, v_s, bias_f, bias_own, bias_all, bfull,
    rs_send, rs_recv, ps_send, ps_recv, as_send, as_recv, bs_send, bs_recv, bf_send,
):
    nrow, ncol, nsub, group = dims
    rows, cols, chan = pair_ref.shape
    cc = ncol * nsub
    residues = cols * cc
    rb = nrow // cc
    nz = nrow // group
    hid = w_gate_ref.shape[1]
    heads = bias_f.shape[0] * 2
    head_size = hid // heads
    ch = next(n for n in (4, 2, 1) if rows % n == 0)
    nt = rows // ch

    r = lax.axis_index("row")
    c = lax.axis_index("col") * nsub + lax.axis_index("sub")
    z = r // group
    p = r % group

    def at(row, cc_index):
        return {"row": row, "col": cc_index // nsub, "sub": cc_index % nsub}

    barrier = pltpu.get_barrier_semaphore()
    me = r * cc + c

    @pl.loop(1, nrow * cc)
    def _(n):
        other = (me + n) % (nrow * cc)
        pl.semaphore_signal(barrier, inc=1, device_id=at(other // cc, other % cc), device_id_type=MESH)

    live = mask_ref[...].astype(F32)
    eye = lax.broadcasted_iota(jnp.int32, (residues, residues), 0) == lax.broadcasted_iota(
        jnp.int32, (residues, residues), 1
    )
    column = jnp.sum(jnp.where(eye, jnp.broadcast_to(live, (residues, residues)), 0.0), axis=1, keepdims=True)
    live_s[...] = jnp.broadcast_to(column, live_s.shape)
    live_cols = live_s[pl.ds(pl.multiple_of(c * cols, 8), cols), :]

    def right_copy(way, slot, t):
        target = (r + group, r - group, z * group + (group - 1 - p))[way]
        piece = right_all.at[slot, pl.ds(t * ch, ch)]
        return pltpu.make_async_remote_copy(
            src_ref=piece, dst_ref=piece,
            send_sem=rs_send.at[way, slot, t], recv_sem=rs_recv.at[slot, t],
            device_id={"row": target}, device_id_type=MESH,
        )

    for t in range(nt):
        sl = slice(t * ch, (t + 1) * ch)
        normed = norm_last(pair_ref[sl].reshape(ch * cols, chan), g1_ref[...]).astype(BF16)
        normed_s[t] = normed
        proj = dot(normed, w_in_ref[:, 2 * hid :])
        prod = (jax.nn.sigmoid(proj[:, :hid]) * proj[:, hid:]).reshape(ch, cols, hid)
        for u in range(ch):
            both = live_cols * live_s[pl.ds(r * rows + t * ch + u, 1), :]
            right_all[r, t * ch + u] = (prod[u] * both).astype(BF16)
        if t == 0:
            pl.semaphore_wait(barrier, nrow * cc - 1)

        @pl.when(z + 1 < nz)
        def _():
            right_copy(0, r, t).start()

        @pl.when(z >= 1)
        def _():
            right_copy(1, r, t).start()

        if group == 2:
            right_copy(2, r, t).start()

    for t in range(nt):
        proj = dot(normed_s[t], w_in_ref[:, : 2 * hid])
        prod = (jax.nn.sigmoid(proj[:, :hid]) * proj[:, hid:]).reshape(ch, cols, hid)
        gate_s[t] = jax.nn.sigmoid(dot(normed_s[t], w_gate_ref[...]))
        for u in range(ch):
            both = live_cols * live_s[pl.ds(r * rows + t * ch + u, 1), :]
            left_s[t * ch + u] = (prod[u] * both).astype(BF16).astype(F32)

    def part_copy(slot, t):
        return pltpu.make_async_remote_copy(
            src_ref=part_s.at[slot, t], dst_ref=part_in.at[c, slot % rb, t],
            send_sem=ps_send.at[slot, t], recv_sem=ps_recv.at[c, slot % rb, t],
            device_id=at(r, slot // rb), device_id_type=MESH,
        )

    ig = next(n for n in (4, 2, 1) if rows % n == 0 and n * ch % 8 == 0)

    def compute(slot, t):
        rf_s[...] = right_all[slot, pl.ds(t * ch, ch)].astype(F32)

        @pl.loop(0, rows // ig)
        def _(ip):
            accs = [None] * (ig * ch)
            for kv in range(cols // 8):
                ks = slice(kv * 8, kv * 8 + 8)
                lefts = [left_s[ip * ig + u, ks, :] for u in range(ig)]
                for j in range(ch):
                    rv = rf_s[j, ks, :]
                    for u in range(ig):
                        n = u * ch + j
                        term = lefts[u] * rv
                        accs[n] = term if accs[n] is None else accs[n] + term
            for n in range(ig * ch // 8):
                start = pl.multiple_of(ip * (ig * ch) + n * 8, 8)
                part_s[slot, t, pl.ds(start, 8), :] = fold_sublanes(accs[n * 8 : n * 8 + 8])

        @pl.when(slot // rb != c)
        def _():
            part_copy(slot, t).start()

    @pl.loop(0, nt)
    def _(t):
        compute(r, t)

    if group == 2:
        @pl.loop(0, nt)
        def _(t):
            right_copy(2, z * group + 1 - p, t).wait_recv()
            compute(z * group + 1 - p, t)

    steps = nt * (nz - 1)

    @pl.loop(0, steps + (1 if group == 2 else 0))
    def _(s):
        away, t = 1 + s // nt, s % nt
        for below in (True, False):
            zn = z - away if below else z + away
            slot = zn * group + p

            @pl.when((s < steps) & (zn >= 0) & (zn < nz))
            def _():
                right_copy(0, slot, t).wait_recv()
                if below:
                    @pl.when(z + 1 < nz)
                    def _():
                        right_copy(0, slot, t).start()
                else:
                    @pl.when(z >= 1)
                    def _():
                        right_copy(1, slot, t).start()
                if group == 2:
                    right_copy(2, slot, t).start()

        @pl.loop(0, 2 * group)
        def _(e):
            old = e // 2
            sq = s - old
            awayq, tq = (sq + nt) // nt, (sq + nt) % nt
            zq = jnp.where(e % 2 == 0, z - awayq, z + awayq)
            slot = zq * group + (p + old) % group

            @pl.when((sq >= 0) & (sq < steps) & (zq >= 0) & (zq < nz))
            def _():
                @pl.when(old == 1)
                def _():
                    right_copy(2, slot, tq).wait_recv()

                compute(slot, tq)

    for b in range(rb):
        for t in range(nt):
            total = part_s[c * rb + b, t]
            for away in range(1, cc):
                source = (c + away) % cc
                pltpu.make_async_remote_copy(
                    src_ref=part_s.at[0, 0], dst_ref=part_in.at[source, b, t],
                    send_sem=ps_send.at[0, 0], recv_sem=ps_recv.at[source, b, t],
                    device_id=at(r, source), device_id_type=MESH,
                ).wait_recv()
                total = total + part_in[source, b, t]
            sum_s[b, t] = total
            first = b * rows + t * ch
            for i in range(rows):
                tri_s[i, first : first + ch, :] = sum_s[b, t, i * ch : (i + 1) * ch, :]

    def att_copy(t, away, source):
        piece = att_all.at[source, pl.ds(t * ch, ch)]
        return pltpu.make_async_remote_copy(
            src_ref=piece, dst_ref=piece,
            send_sem=as_send.at[away, t], recv_sem=as_recv.at[source, t],
            device_id=at(r, (c + away) % cc), device_id_type=MESH,
        )

    bias_f[...] = jnp.zeros_like(bias_f)
    for t in range(nt):
        sl = slice(t * ch, (t + 1) * ch)
        hidden = norm_last(tri_s[sl].reshape(ch * cols, hid), g2_ref[...]).astype(BF16)
        mid = pair_ref[sl].reshape(ch * cols, chan) + gate_s[t] * dot(hidden, w_out_ref[...])
        mid_s[t] = mid
        att = norm_last(mid, g3_ref[...]).astype(BF16)
        att_all[c, sl] = att.reshape(ch, cols, chan)
        if t < nt - 1:
            for away in range(1, cc):
                att_copy(t, away, c).start()
        for u in range(ch):
            heads_first = dot_nt(w_bias_ref[...], att[u * cols : (u + 1) * cols])
            for h in range(heads):
                at_lane = h % 2 * cols
                bias_f[h // 2, t * ch + u : t * ch + u + 1, at_lane : at_lane + cols] = heads_first[h : h + 1, :]

    bias_own[...] = bias_f[...].astype(BF16)
    panel = r // rb

    def bias_copy(row, source_c, source_b):
        return pltpu.make_async_remote_copy(
            src_ref=bias_own, dst_ref=bias_all.at[source_c, source_b],
            send_sem=bs_send.at[row], recv_sem=bs_recv.at[source_c, source_b],
            device_id=at(row, panel), device_id_type=MESH,
        )

    @pl.loop(0, nz)
    def _(n):
        row = (z + n) % nz * group + p

        @pl.when((n > 0) | (panel != c))
        def _():
            bias_copy(row, c, r % rb).start()

    for away in range(1, cc):
        att_copy(nt - 1, away, c).start()

    @pl.when(panel == c)
    def _():
        bias_all[c, r % rb] = bias_f[...].astype(BF16)

    for t in range(nt):
        sl = slice(t * ch, (t + 1) * ch)
        att = att_all[c, sl].reshape(ch * cols, chan)
        proj = dot(att, w_att_ref[...])
        q_s[sl] = (proj[:, :hid] * head_size ** (-0.5)).astype(BF16).reshape(ch, cols, hid)
        k_s[c, sl] = proj[:, hid : 2 * hid].astype(BF16).reshape(ch, cols, hid)
        v_s[c, sl] = proj[:, 2 * hid : 3 * hid].astype(BF16).reshape(ch, cols, hid)
        ag_s[sl] = jax.nn.sigmoid(proj[:, 3 * hid :]).reshape(ch, cols, hid)

    def bias_pass(source, b):
        return pltpu.make_async_remote_copy(
            src_ref=bias_all.at[source, b], dst_ref=bias_all.at[source, b],
            send_sem=bf_send.at[source, b], recv_sem=bs_recv.at[source, b],
            device_id={"row": z * group + (group - 1 - p)}, device_id_type=MESH,
        )

    for source in range(cc):
        for b in range(rb):
            @pl.when((c * rb + b) % group == p)
            def _():
                @pl.when((c != source) | (r != c * rb + b))
                def _():
                    bias_copy(r, source, b).wait_recv()

                if group == 2:
                    bias_pass(source, b).start()

    for away in range(1, cc):
        source = (c + away) % cc
        for t in range(nt):
            sl = slice(t * ch, (t + 1) * ch)
            att_copy(t, away, source).wait_recv()
            att = att_all[source, sl].reshape(ch * cols, chan)
            proj = dot(att, w_att_ref[:, hid : 3 * hid])
            k_s[source, sl] = proj[:, :hid].astype(BF16).reshape(ch, cols, hid)
            v_s[source, sl] = proj[:, hid:].astype(BF16).reshape(ch, cols, hid)

    mask_row = (live - 1.0) * mask_penalty
    for source in range(cc):
        for b in range(rb):
            @pl.when((c * rb + b) % group != p)
            def _():
                bias_copy(r, source, b).wait_recv()

            for h in range(heads):
                bfull[h, b * rows : (b + 1) * rows, source * cols : (source + 1) * cols] = (
                    bias_all[source, b, h // 2].astype(F32)[:rows, h % 2 * cols : (h % 2 + 1) * cols] + mask_row[:, source * cols : (source + 1) * cols]
                )

    head_of = lax.broadcasted_iota(jnp.int32, (cols, hid), 1) // head_size
    ones = jnp.ones((residues, hid), BF16)

    @pl.loop(0, nt)
    def _(t):
        gated = []
        for u in range(ch):
            i = t * ch + u
            query = q_s[i]
            stacked = jnp.concatenate(
                [jnp.where(head_of == h, query, jnp.zeros_like(query)) for h in range(heads)], axis=0
            )
            keys = jnp.concatenate([k_s[s, i] for s in range(cc)], axis=0)
            values = jnp.concatenate([v_s[s, i] for s in range(cc)], axis=0)
            scores = dot_nt(stacked, keys) + bfull[...].reshape(heads * cols, residues)
            raised = jnp.exp(scores - jnp.max(scores, axis=-1, keepdims=True)).astype(BF16)
            both = dot(raised, jnp.concatenate([values, ones], axis=1))
            top, bottom = both[:cols, :hid], both[:cols, hid:]
            for h in range(1, heads):
                rows_h = both[h * cols : (h + 1) * cols]
                top = jnp.where(head_of == h, rows_h[:, :hid], top)
                bottom = jnp.where(head_of == h, rows_h[:, hid:], bottom)
            gated.append((top / bottom * ag_s[i]).astype(BF16))
        result = mid_s[t] + dot(jnp.concatenate(gated, axis=0), w_o_ref[...])
        out_ref[pl.ds(t * ch, ch)] = result.reshape(ch, cols, chan)

    @pl.loop(0, nrow)
    def _(slot):
        zn, pn = slot // group, slot % group

        @pl.when(pn == p)
        def _():
            for t in range(nt):
                @pl.when((zn <= z) & (z + 1 < nz))
                def _():
                    right_copy(0, slot, t).wait_send()

                @pl.when((zn >= z) & (z >= 1))
                def _():
                    right_copy(1, slot, t).wait_send()

                if group == 2:
                    right_copy(2, slot, t).wait_send()

        @pl.when(slot // rb != c)
        def _():
            for t in range(nt):
                part_copy(slot, t).wait_send()

        @pl.when((pn == p) & ((slot != r) | (panel != c)))
        def _():
            bias_copy(slot, c, r % rb).wait_send()

    if group == 2:
        for source in range(cc):
            for b in range(rb):
                @pl.when((c * rb + b) % group == p)
                def _():
                    bias_pass(source, b).wait_send()

    for away in range(1, cc):
        for t in range(nt):
            att_copy(t, away, c).wait_send()


def body(dims, pair, residue_mask, g1, w_in, w_gate, g2, w_out, g3, w_att, w_bias, w_o):
    nrow, ncol, nsub, group = dims
    rows, cols, chan = pair.shape
    cc = ncol * nsub
    residues = cols * cc
    rb = nrow // cc
    hid = w_in.shape[2]
    heads = w_bias.shape[1]
    ch = next(n for n in (4, 2, 1) if rows % n == 0)
    nt = rows // ch
    pad = -(-rows // 16) * 16
    bias_rows = jnp.pad(w_bias.T, ((0, -heads % 16), (0, 0)))
    V = pltpu.VMEM
    DMA = pltpu.SemaphoreType.DMA
    return pl.pallas_call(
        functools.partial(kernel, dims),
        out_shape=jax.ShapeDtypeStruct(pair.shape, F32),
        in_specs=[pl.BlockSpec(memory_space=pltpu.VMEM)] * 11,
        out_specs=pl.BlockSpec(memory_space=pltpu.VMEM),
        scratch_shapes=[
            V((residues, hid), F32),
            V((nt, ch * cols, chan), BF16),
            V((nrow, rows, cols, hid), BF16),
            V((rows, cols, hid), F32),
            V((nt, ch * cols, chan), F32),
            V((ch, cols, hid), F32),
            V((nrow, nt, rows * ch, hid), F32),
            V((cc, rb, nt, rows * ch, hid), F32),
            V((rb, nt, rows * ch, hid), F32),
            V((rows, cols, hid), F32),
            V((nt, ch * cols, chan), F32),
            V((cc, rows, cols, chan), BF16),
            V((rows, cols, hid), BF16),
            V((rows, cols, hid), F32),
            V((cc, rows, cols, hid), BF16),
            V((cc, rows, cols, hid), BF16),
            V((heads // 2, pad, 2 * cols), F32),
            V((heads // 2, pad, 2 * cols), BF16),
            V((cc, rb, heads // 2, pad, 2 * cols), BF16),
            V((heads, cols, residues), F32),
            DMA((3, nrow, nt)),
            DMA((nrow, nt)),
            DMA((nrow, nt)),
            DMA((cc, rb, nt)),
            DMA((cc, nt)),
            DMA((cc, nt)),
            DMA((nrow,)),
            DMA((cc, rb)),
            DMA((cc, rb)),
        ],
        compiler_params=pltpu.CompilerParams(
            collective_id=0, has_side_effects=True, vmem_limit_bytes=56 * 1024 * 1024
        ),
        name="pair_update",
    )(
        pair,
        residue_mask.reshape(1, -1),
        g1.reshape(1, -1),
        w_in.reshape(chan, -1),
        w_gate,
        g2.reshape(1, -1),
        w_out,
        g3.reshape(1, -1),
        w_att.reshape(chan, -1),
        bias_rows,
        w_o,
    )


def solution(mesh):
    shape = mesh.shape
    group = 2 if shape["sub"] == 1 and shape["row"] % 2 == 0 else 1
    dims = (shape["row"], shape["col"], shape["sub"], group)
    placed = (P(("parts", "row"), ("col", "sub"), None), P("parts")) + (P(),) * 9
    return jax.shard_map(
        functools.partial(body, dims),
        mesh=mesh,
        in_specs=placed,
        out_specs=P(("parts", "row"), ("col", "sub"), None),
        check_vma=False,
    )
```

```python
import functools
import math

import jax
import jax.numpy as jnp
from jax import lax
from jax.experimental import pallas as pl
from jax.experimental.pallas import tpu as pltpu
from jax.sharding import PartitionSpec as P

epsilon = 1e-05
mask_penalty = 1000000000.0
MESH = pl.DeviceIdType.MESH
F32 = jnp.float32
BF16 = jnp.bfloat16


def norm_last(values_in, gain):
    center = jnp.mean(values_in, axis=-1, keepdims=True)
    centered = values_in - center
    variance = jnp.mean(centered * centered, axis=-1, keepdims=True)
    return centered * lax.rsqrt(variance + epsilon) * gain


def dot(a, b):
    return jnp.dot(a, b, preferred_element_type=F32)


def dot_nt(a, b):
    return lax.dot_general(a, b, (((1,), (1,)), ((), ())), preferred_element_type=F32)


def fold_sublanes(parts):
    lane_row = lax.broadcasted_iota(jnp.int32, parts[0].shape, 0)
    for width in (4, 2, 1):
        low = (lane_row & width) == 0
        half = len(parts) // 2
        folded = []
        for u in range(half):
            x, y = parts[u], parts[u + half]
            if width == 4:
                folded.append(jnp.where(low, x, y) + pltpu.roll(jnp.where(low, y, x), 4, 0))
            else:
                folded.append(
                    jnp.where(low, x, y)
                    + jnp.where(low, pltpu.roll(x, 8 - width, 0), pltpu.roll(y, width, 0))
                )
        parts = folded
    return parts[0]


def kernel(
    dims,
    pair_ref, mask_ref, g1_ref, w_in3_ref, w_gate_ref, g2_ref, w_out_ref, g3_ref, w_att3_ref, w_bias_ref, w_o_ref,
    out_ref,
    live_s, normed_s, right_all, left_s, gate_s, rf_s, part_s, part_in, sum_s, tri_s, mid_s,
    att_all, q_s, ag_s, k_s, v_s, bias_f, bias_own, bias_all, bfull,
    rs_send, rs_recv, ps_send, ps_recv, as_send, as_recv, bs_send, bs_recv, bf_send, w_in_ref, w_att_ref, wide_s,
):
    nrow, ncol, nsub, group = dims
    rows, cols, chan = pair_ref.shape
    cc = ncol * nsub
    residues = cols * cc
    rb = nrow // cc
    nz = nrow // group
    hid = w_gate_ref.shape[1]
    heads = bias_f.shape[0] * 2
    head_size = hid // heads
    ch = next(n for n in (4, 2, 1) if rows % n == 0)
    nt = rows // ch

    r = lax.axis_index("row")
    c = lax.axis_index("col") * nsub + lax.axis_index("sub")
    z = r // group
    p = r % group

    def at(row, cc_index):
        return {"row": row, "col": cc_index // nsub, "sub": cc_index % nsub}

    def spread(w_ref, flat_ref):
        for n in range(chan):
            wide_s[n * 4 : n * 4 + 4, :] = w_ref[n].astype(F32)
        for n in range(4):
            flat_ref[:, n * hid : (n + 1) * hid] = wide_s[pl.ds(n, chan, stride=4), :].astype(BF16)

    barrier = pltpu.get_barrier_semaphore()
    me = r * cc + c

    @pl.loop(1, nrow * cc)
    def _(n):
        other = (me + n) % (nrow * cc)
        pl.semaphore_signal(barrier, inc=1, device_id=at(other // cc, other % cc), device_id_type=MESH)

    spread(w_in3_ref, w_in_ref)

    live = mask_ref[...].astype(F32)
    eye = lax.broadcasted_iota(jnp.int32, (residues, residues), 0) == lax.broadcasted_iota(
        jnp.int32, (residues, residues), 1
    )
    column = jnp.sum(jnp.where(eye, jnp.broadcast_to(live, (residues, residues)), 0.0), axis=1, keepdims=True)
    live_s[...] = jnp.broadcast_to(column, live_s.shape)
    live_cols = live_s[pl.ds(pl.multiple_of(c * cols, 8), cols), :]

    def right_copy(way, slot, t):
        target = (r + group, r - group, z * group + (group - 1 - p))[way]
        piece = right_all.at[slot, pl.ds(t * ch, ch)]
        return pltpu.make_async_remote_copy(
            src_ref=piece, dst_ref=piece,
            send_sem=rs_send.at[way, slot, t], recv_sem=rs_recv.at[slot, t],
            device_id={"row": target}, device_id_type=MESH,
        )

    for t in range(nt):
        sl = slice(t * ch, (t + 1) * ch)
        normed = norm_last(pair_ref[sl].reshape(ch * cols, chan), g1_ref[...]).astype(BF16)
        normed_s[t] = normed
        proj = dot(normed, w_in_ref[:, 2 * hid :])
        prod = (jax.nn.sigmoid(proj[:, :hid]) * proj[:, hid:]).reshape(ch, cols, hid)
        for u in range(ch):
            both = live_cols * live_s[pl.ds(r * rows + t * ch + u, 1), :]
            right_all[r, t * ch + u] = (prod[u] * both).astype(BF16)
        if t == 0:
            pl.semaphore_wait(barrier, nrow * cc - 1)

        @pl.when(z + 1 < nz)
        def _():
            right_copy(0, r, t).start()

        @pl.when(z >= 1)
        def _():
            right_copy(1, r, t).start()

        if group == 2:
            right_copy(2, r, t).start()

    for t in range(nt):
        proj = dot(normed_s[t], w_in_ref[:, : 2 * hid])
        prod = (jax.nn.sigmoid(proj[:, :hid]) * proj[:, hid:]).reshape(ch, cols, hid)
        gate_s[t] = jax.nn.sigmoid(dot(normed_s[t], w_gate_ref[...]))
        for u in range(ch):
            both = live_cols * live_s[pl.ds(r * rows + t * ch + u, 1), :]
            left_s[t * ch + u] = (prod[u] * both).astype(BF16).astype(F32)

    def part_copy(slot, t):
        return pltpu.make_async_remote_copy(
            src_ref=part_s.at[slot, t], dst_ref=part_in.at[c, slot % rb, t],
            send_sem=ps_send.at[slot, t], recv_sem=ps_recv.at[c, slot % rb, t],
            device_id=at(r, slot // rb), device_id_type=MESH,
        )

    spread(w_att3_ref, w_att_ref)
    ig = next(n for n in (4, 2, 1) if rows % n == 0 and n * ch % 8 == 0)

    def compute(slot, t):
        rf_s[...] = right_all[slot, pl.ds(t * ch, ch)].astype(F32)

        @pl.loop(0, rows // ig)
        def _(ip):
            accs = [None] * (ig * ch)
            for kv in range(cols // 8):
                ks = slice(kv * 8, kv * 8 + 8)
                lefts = [left_s[ip * ig + u, ks, :] for u in range(ig)]
                for j in range(ch):
                    rv = rf_s[j, ks, :]
                    for u in range(ig):
                        n = u * ch + j
                        term = lefts[u] * rv
                        accs[n] = term if accs[n] is None else accs[n] + term
            for n in range(ig * ch // 8):
                start = pl.multiple_of(ip * (ig * ch) + n * 8, 8)
                part_s[slot, t, pl.ds(start, 8), :] = fold_sublanes(accs[n * 8 : n * 8 + 8])

        @pl.when(slot // rb != c)
        def _():
            part_copy(slot, t).start()

    @pl.loop(0, nt)
    def _(t):
        compute(r, t)

    if group == 2:
        @pl.loop(0, nt)
        def _(t):
            right_copy(2, z * group + 1 - p, t).wait_recv()
            compute(z * group + 1 - p, t)

    steps = nt * (nz - 1)

    @pl.loop(0, steps + (1 if group == 2 else 0))
    def _(s):
        away, t = 1 + s // nt, s % nt
        for below in (True, False):
            zn = z - away if below else z + away
            slot = zn * group + p

            @pl.when((s < steps) & (zn >= 0) & (zn < nz))
            def _():
                right_copy(0, slot, t).wait_recv()
                if below:
                    @pl.when(z + 1 < nz)
                    def _():
                        right_copy(0, slot, t).start()
                else:
                    @pl.when(z >= 1)
                    def _():
                        right_copy(1, slot, t).start()
                if group == 2:
                    right_copy(2, slot, t).start()

        @pl.loop(0, 2 * group)
        def _(e):
            old = e // 2
            sq = s - old
            awayq, tq = (sq + nt) // nt, (sq + nt) % nt
            zq = jnp.where(e % 2 == 0, z - awayq, z + awayq)
            slot = zq * group + (p + old) % group

            @pl.when((sq >= 0) & (sq < steps) & (zq >= 0) & (zq < nz))
            def _():
                @pl.when(old == 1)
                def _():
                    right_copy(2, slot, tq).wait_recv()

                compute(slot, tq)

    for b in range(rb):
        for t in range(nt):
            total = part_s[c * rb + b, t]
            for away in range(1, cc):
                source = (c + away) % cc
                pltpu.make_async_remote_copy(
                    src_ref=part_s.at[0, 0], dst_ref=part_in.at[source, b, t],
                    send_sem=ps_send.at[0, 0], recv_sem=ps_recv.at[source, b, t],
                    device_id=at(r, source), device_id_type=MESH,
                ).wait_recv()
                total = total + part_in[source, b, t]
            sum_s[b, t] = total
            first = b * rows + t * ch
            for i in range(rows):
                tri_s[i, first : first + ch, :] = sum_s[b, t, i * ch : (i + 1) * ch, :]

    def att_copy(t, away, source):
        piece = att_all.at[source, pl.ds(t * ch, ch)]
        return pltpu.make_async_remote_copy(
            src_ref=piece, dst_ref=piece,
            send_sem=as_send.at[away, t], recv_sem=as_recv.at[source, t],
            device_id=at(r, (c + away) % cc), device_id_type=MESH,
        )

    bias_f[...] = jnp.zeros_like(bias_f)
    for t in range(nt):
        sl = slice(t * ch, (t + 1) * ch)
        hidden = norm_last(tri_s[sl].reshape(ch * cols, hid), g2_ref[...]).astype(BF16)
        mid = pair_ref[sl].reshape(ch * cols, chan) + gate_s[t] * dot(hidden, w_out_ref[...])
        mid_s[t] = mid
        att = norm_last(mid, g3_ref[...]).astype(BF16)
        att_all[c, sl] = att.reshape(ch, cols, chan)
        if t < nt - 1:
            for away in range(1, cc):
                att_copy(t, away, c).start()
        for u in range(ch):
            heads_first = dot_nt(w_bias_ref[...], att[u * cols : (u + 1) * cols])
            for h in range(heads):
                at_lane = h % 2 * cols
                bias_f[h // 2, t * ch + u : t * ch + u + 1, at_lane : at_lane + cols] = heads_first[h : h + 1, :]

    bias_own[...] = bias_f[...].astype(BF16)
    panel = r // rb

    def bias_copy(row, source_c, source_b):
        return pltpu.make_async_remote_copy(
            src_ref=bias_own, dst_ref=bias_all.at[source_c, source_b],
            send_sem=bs_send.at[row], recv_sem=bs_recv.at[source_c, source_b],
            device_id=at(row, panel), device_id_type=MESH,
        )

    @pl.loop(0, nz)
    def _(n):
        row = (z + n) % nz * group + p

        @pl.when((n > 0) | (panel != c))
        def _():
            bias_copy(row, c, r % rb).start()

    for away in range(1, cc):
        att_copy(nt - 1, away, c).start()

    @pl.when(panel == c)
    def _():
        bias_all[c, r % rb] = bias_f[...].astype(BF16)

    for t in range(nt):
        sl = slice(t * ch, (t + 1) * ch)
        att = att_all[c, sl].reshape(ch * cols, chan)
        proj = dot(att, w_att_ref[...])
        q_s[sl] = (proj[:, :hid] * head_size ** (-0.5)).astype(BF16).reshape(ch, cols, hid)
        k_s[c, sl] = proj[:, hid : 2 * hid].astype(BF16).reshape(ch, cols, hid)
        v_s[c, sl] = proj[:, 2 * hid : 3 * hid].astype(BF16).reshape(ch, cols, hid)
        ag_s[sl] = jax.nn.sigmoid(proj[:, 3 * hid :]).reshape(ch, cols, hid)

    def bias_pass(source, b):
        return pltpu.make_async_remote_copy(
            src_ref=bias_all.at[source, b], dst_ref=bias_all.at[source, b],
            send_sem=bf_send.at[source, b], recv_sem=bs_recv.at[source, b],
            device_id={"row": z * group + (group - 1 - p)}, device_id_type=MESH,
        )

    for source in range(cc):
        for b in range(rb):
            @pl.when((c * rb + b) % group == p)
            def _():
                @pl.when((c != source) | (r != c * rb + b))
                def _():
                    bias_copy(r, source, b).wait_recv()

                if group == 2:
                    bias_pass(source, b).start()

    for away in range(1, cc):
        source = (c + away) % cc
        for t in range(nt):
            sl = slice(t * ch, (t + 1) * ch)
            att_copy(t, away, source).wait_recv()
            att = att_all[source, sl].reshape(ch * cols, chan)
            proj = dot(att, w_att_ref[:, hid : 3 * hid])
            k_s[source, sl] = proj[:, :hid].astype(BF16).reshape(ch, cols, hid)
            v_s[source, sl] = proj[:, hid:].astype(BF16).reshape(ch, cols, hid)

    mask_row = (live - 1.0) * mask_penalty
    for source in range(cc):
        for b in range(rb):
            @pl.when((c * rb + b) % group != p)
            def _():
                bias_copy(r, source, b).wait_recv()

            for h in range(heads):
                bfull[h, b * rows : (b + 1) * rows, source * cols : (source + 1) * cols] = (
                    bias_all[source, b, h // 2].astype(F32)[:rows, h % 2 * cols : (h % 2 + 1) * cols] + mask_row[:, source * cols : (source + 1) * cols]
                )

    head_of = lax.broadcasted_iota(jnp.int32, (cols, hid), 1) // head_size
    ones = jnp.ones((residues, hid), BF16)

    @pl.loop(0, nt)
    def _(t):
        gated = []
        for u in range(ch):
            i = t * ch + u
            query = q_s[i]
            stacked = jnp.concatenate(
                [jnp.where(head_of == h, query, jnp.zeros_like(query)) for h in range(heads)], axis=0
            )
            keys = jnp.concatenate([k_s[s, i] for s in range(cc)], axis=0)
            values = jnp.concatenate([v_s[s, i] for s in range(cc)], axis=0)
            scores = dot_nt(stacked, keys) + bfull[...].reshape(heads * cols, residues)
            raised = jnp.exp(scores - jnp.max(scores, axis=-1, keepdims=True)).astype(BF16)
            both = dot(raised, jnp.concatenate([values, ones], axis=1))
            top, bottom = both[:cols, :hid], both[:cols, hid:]
            for h in range(1, heads):
                rows_h = both[h * cols : (h + 1) * cols]
                top = jnp.where(head_of == h, rows_h[:, :hid], top)
                bottom = jnp.where(head_of == h, rows_h[:, hid:], bottom)
            gated.append((top / bottom * ag_s[i]).astype(BF16))
        result = mid_s[t] + dot(jnp.concatenate(gated, axis=0), w_o_ref[...])
        out_ref[pl.ds(t * ch, ch)] = result.reshape(ch, cols, chan)

    @pl.loop(0, nrow)
    def _(slot):
        zn, pn = slot // group, slot % group

        @pl.when(pn == p)
        def _():
            for t in range(nt):
                @pl.when((zn <= z) & (z + 1 < nz))
                def _():
                    right_copy(0, slot, t).wait_send()

                @pl.when((zn >= z) & (z >= 1))
                def _():
                    right_copy(1, slot, t).wait_send()

                if group == 2:
                    right_copy(2, slot, t).wait_send()

        @pl.when(slot // rb != c)
        def _():
            for t in range(nt):
                part_copy(slot, t).wait_send()

        @pl.when((pn == p) & ((slot != r) | (panel != c)))
        def _():
            bias_copy(slot, c, r % rb).wait_send()

    if group == 2:
        for source in range(cc):
            for b in range(rb):
                @pl.when((c * rb + b) % group == p)
                def _():
                    bias_pass(source, b).wait_send()

    for away in range(1, cc):
        for t in range(nt):
            att_copy(t, away, c).wait_send()


def body(dims, pair, residue_mask, g1, w_in, w_gate, g2, w_out, g3, w_att, w_bias, w_o):
    nrow, ncol, nsub, group = dims
    rows, cols, chan = pair.shape
    cc = ncol * nsub
    residues = cols * cc
    rb = nrow // cc
    hid = w_in.shape[2]
    heads = w_bias.shape[1]
    ch = next(n for n in (4, 2, 1) if rows % n == 0)
    nt = rows // ch
    pad = -(-rows // 16) * 16
    V = pltpu.VMEM
    DMA = pltpu.SemaphoreType.DMA
    return pl.pallas_call(
        functools.partial(kernel, dims),
        out_shape=jax.ShapeDtypeStruct(pair.shape, F32),
        in_specs=[pl.BlockSpec(memory_space=pltpu.VMEM)] * 11,
        out_specs=pl.BlockSpec(memory_space=pltpu.VMEM),
        scratch_shapes=[
            V((residues, hid), F32),
            V((nt, ch * cols, chan), BF16),
            V((nrow, rows, cols, hid), BF16),
            V((rows, cols, hid), F32),
            V((nt, ch * cols, chan), F32),
            V((ch, cols, hid), F32),
            V((nrow, nt, rows * ch, hid), F32),
            V((cc, rb, nt, rows * ch, hid), F32),
            V((rb, nt, rows * ch, hid), F32),
            V((rows, cols, hid), F32),
            V((nt, ch * cols, chan), F32),
            V((cc, rows, cols, chan), BF16),
            V((rows, cols, hid), BF16),
            V((rows, cols, hid), F32),
            V((cc, rows, cols, hid), BF16),
            V((cc, rows, cols, hid), BF16),
            V((heads // 2, pad, 2 * cols), F32),
            V((heads // 2, pad, 2 * cols), BF16),
            V((cc, rb, heads // 2, pad, 2 * cols), BF16),
            V((heads, cols, residues), F32),
            DMA((3, nrow, nt)),
            DMA((nrow, nt)),
            DMA((nrow, nt)),
            DMA((cc, rb, nt)),
            DMA((cc, nt)),
            DMA((cc, nt)),
            DMA((nrow,)),
            DMA((cc, rb)),
            DMA((cc, rb)),
            V((chan, 4 * hid), BF16),
            V((chan, 4 * hid), BF16),
            V((4 * chan, hid), F32),
        ],
        compiler_params=pltpu.CompilerParams(
            collective_id=0, has_side_effects=True, vmem_limit_bytes=56 * 1024 * 1024
        ),
        name="pair_update",
    )(
        pair,
        residue_mask.reshape(1, -1),
        g1.reshape(1, -1),
        w_in,
        w_gate,
        g2.reshape(1, -1),
        w_out,
        g3.reshape(1, -1),
        w_att,
        w_bias.T,
        w_o,
    )


def solution(mesh):
    shape = mesh.shape
    group = 2 if shape["sub"] == 1 and shape["row"] % 2 == 0 else 1
    dims = (shape["row"], shape["col"], shape["sub"], group)
    placed = (P(("parts", "row"), ("col", "sub"), None), P("parts")) + (P(),) * 9
    return jax.shard_map(
        functools.partial(body, dims),
        mesh=mesh,
        in_specs=placed,
        out_specs=P(("parts", "row"), ("col", "sub"), None),
        check_vma=False,
    )
```
